64 devices in a mesh: rep: 4 (over x, y), dp: 16 (over z, core).
Axes of the slice: x: 2, y: 2, z: 8, core: 2. Of those that a mesh axis runs over, the one named last changes fastest.
The devices are a block of a 4x4x8 slice.
Arguments:
- x: bfloat16 [64, 2048, 512], P(('rep', 'dp')), parts along dimension 0
- dy: bfloat16 [64, 2048, 512], P(('rep', 'dp')), parts along dimension 0
- wq: bfloat16 [2, 512, 512], P(None, 'dp')
- wk: bfloat16 [2, 512, 512], P(None, 'dp')
- wv: bfloat16 [2, 512, 512], P(None, 'dp')
- wo: bfloat16 [2, 512, 512], P(None, 'dp')
- w_gate: bfloat16 [2, 512, 2048], P(None, 'dp')
- w_up: bfloat16 [2, 512, 2048], P(None, 'dp')
- w_down: bfloat16 [2, 2048, 512], P(None, 'dp')
- m_wq: float32 [2, 512, 512], P(None, 'dp')
- m_wk: float32 [2, 512, 512], P(None, 'dp')
- m_wv: float32 [2, 512, 512], P(None, 'dp')
- m_wo: float32 [2, 512, 512], P(None, 'dp')
- m_w_gate: float32 [2, 512, 2048], P(None, 'dp')
- m_w_up: float32 [2, 512, 2048], P(None, 'dp')
- m_w_down: float32 [2, 2048, 512], P(None, 'dp')
- v_wq: float32 [2, 512, 512], P(None, 'dp')
- v_wk: float32 [2, 512, 512], P(None, 'dp')
- v_wv: float32 [2, 512, 512], P(None, 'dp')
- v_wo: float32 [2, 512, 512], P(None, 'dp')
- v_w_gate: float32 [2, 512, 2048], P(None, 'dp')
- v_w_up: float32 [2, 512, 2048], P(None, 'dp')
- v_w_down: float32 [2, 2048, 512], P(None, 'dp')
Outputs:
- output 1: bfloat16 [8, 512, 512], P('rep', 'dp'), parts along dimension 0
- output 2: bfloat16 [8, 512, 512], P('rep', 'dp'), parts along dimension 0
- output 3: bfloat16 [8, 512, 512], P('rep', 'dp'), parts along dimension 0
- output 4: bfloat16 [8, 512, 512], P('rep', 'dp'), parts along dimension 0
- output 5: bfloat16 [8, 512, 2048], P('rep', 'dp'), parts along dimension 0
- output 6: bfloat16 [8, 512, 2048], P('rep', 'dp'), parts along dimension 0
- output 7: bfloat16 [8, 2048, 512], P('rep', 'dp'), parts along dimension 0
- output 8: float32 [8, 512, 512], P('rep', 'dp'), parts along dimension 0
- output 9: float32 [8, 512, 512], P('rep', 'dp'), parts along dimension 0
- output 10: float32 [8, 512, 512], P('rep', 'dp'), parts along dimension 0
- output 11: float32 [8, 512, 512], P('rep', 'dp'), parts along dimension 0
- output 12: float32 [8, 512, 2048], P('rep', 'dp'), parts along dimension 0
- output 13: float32 [8, 512, 2048], P('rep', 'dp'), parts along dimension 0
- output 14: float32 [8, 2048, 512], P('rep', 'dp'), parts along dimension 0
- output 15: float32 [8, 512, 512], P('rep', 'dp'), parts along dimension 0
- output 16: float32 [8, 512, 512], P('rep', 'dp'), parts along dimension 0
- output 17: float32 [8, 512, 512], P('rep', 'dp'), parts along dimension 0
- output 18: float32 [8, 512, 512], P('rep', 'dp'), parts along dimension 0
- output 19: float32 [8, 512, 2048], P('rep', 'dp'), parts along dimension 0
- output 20: float32 [8, 512, 2048], P('rep', 'dp'), parts along dimension 0
- output 21: float32 [8, 2048, 512], P('rep', 'dp'), parts along dimension 0
There are 4 independent parts. The reference program is written for one: setup_inputs(seed, part) draws one part's arguments, and reference() takes and returns one part's arrays. A program takes and returns all parts, laid end to end along the dimension named above; an argument that names none is the same for every part.
All inputs are finite; a program needn't handle non-finite values.
Results may differ from the reference program's by a relative error of at most 0.0241.
Values are sent between devices in bfloat16 or wider.
A program may use at most 768 MiB of HBM per device.

```python
import jax
import jax.numpy as jnp
from jax import lax

SEQUENCES = 16
TOKENS = 2048
D = 512
HEADS = 4
KV_HEADS = 4
HEAD = 128
FF = 2048
LAYERS = 2
THETA = 10000
NAMES = ("wq", "wk", "wv", "wo", "w_gate", "w_up", "w_down")
SHAPES = {
    "wq": (LAYERS, D, HEADS * HEAD),
    "wk": (LAYERS, D, KV_HEADS * HEAD),
    "wv": (LAYERS, D, KV_HEADS * HEAD),
    "wo": (LAYERS, HEADS * HEAD, D),
    "w_gate": (LAYERS, D, FF),
    "w_up": (LAYERS, D, FF),
    "w_down": (LAYERS, FF, D),
}


def bump(key, n, height):
    away = (jnp.arange(n, dtype=jnp.int32) - jax.random.randint(key, (), 0, n, jnp.int32)) % n
    return jnp.where(away < n // 8, height, 1.0)


def together(key, own, strength):
    shared = jax.random.normal(key, own.shape[1:], jnp.float32)
    return (own + strength * shared) * lax.rsqrt(1 + strength * strength)


def setup_inputs(seed: int = 0, part: int = 0) -> dict:
    kx, kdy, ka, kb, kz, kf, kh, kl, *keys = jax.random.split(jax.random.key(seed), 8 + 3 * len(NAMES))
    kx, kdy, ka, kb = (jax.random.fold_in(k, part) for k in (kx, kdy, ka, kb))
    kw, km, kv = (keys[i::3] for i in range(3))
    shape = (SEQUENCES, TOKENS, D)
    much_x, much_dy = jax.random.uniform(kz, (2,), jnp.float32, 0.0, 1.0)
    loud = 2.0 ** jax.random.uniform(jax.random.fold_in(kz, 1), (), jnp.float32, -1.0, 2.0)
    layers = 2.0 ** jax.random.uniform(kl, (LAYERS, 1, 1), jnp.float32, -1.0, 1.0)
    times = {"wq": 1.0, "wk": 1.0, "wv": 2.0, "wo": layers, "w_gate": 1.0, "w_up": bump(kh, FF, 4.0), "w_down": layers}
    x = together(ka, jax.random.normal(kx, shape, jnp.float32), much_x) * bump(kf, D, 4.0)
    dy = together(kb, jax.random.normal(kdy, shape, jnp.float32), much_dy)
    drawn = {"x": x.astype(jnp.bfloat16), "dy": (loud * dy * (SEQUENCES * TOKENS) ** -0.5).astype(jnp.bfloat16)}
    for key, name in zip(kw, NAMES, strict=True):
        drawn[name] = (jax.random.normal(key, SHAPES[name], jnp.float32) * SHAPES[name][1] ** -0.5 * times[name]).astype(jnp.bfloat16)
    for key, name in zip(km, NAMES, strict=True):
        drawn[f"m_{name}"] = 0.1 * jax.random.normal(key, SHAPES[name], jnp.float32)
    for key, name in zip(kv, NAMES, strict=True):
        drawn[f"v_{name}"] = jax.random.uniform(key, SHAPES[name], jnp.float32, 0.02, 0.06)
    return drawn


def matmul(a, w):
    return jnp.dot(a, w, preferred_element_type=jnp.float32).astype(jnp.bfloat16)


def normed(h):
    wide = h.astype(jnp.float32)
    scale = lax.rsqrt(jnp.mean(wide**2, -1, keepdims=True) + 1e-6)
    return (wide * scale).astype(jnp.bfloat16)


def turned(t, theta):
    half = t.shape[-1] // 2
    angle = jnp.arange(t.shape[0], dtype=jnp.float32)[:, None] * theta ** (-jnp.arange(half, dtype=jnp.float32) / half)
    cos, sin = jnp.cos(angle)[:, None], jnp.sin(angle)[:, None]
    a, b = t[..., :half].astype(jnp.float32), t[..., half:].astype(jnp.float32)
    return jnp.concatenate([a * cos - b * sin, b * cos + a * sin], -1).astype(jnp.bfloat16)


def seen_by(q, k, v):
    tokens, kv = q.shape[0], k.shape[1]
    q = q.reshape(tokens, kv, -1, q.shape[-1])
    scores = jnp.einsum("tgsd,ugd->gstu", q.astype(jnp.float32), k.astype(jnp.float32)) * q.shape[-1] ** -0.5
    place = jnp.arange(tokens)
    weights = jax.nn.softmax(jnp.where(place[:, None] >= place, scores, -jnp.inf), -1).astype(jnp.bfloat16)
    return jnp.einsum("gstu,ugd->tgsd", weights.astype(jnp.float32), v.astype(jnp.float32)).astype(jnp.bfloat16).reshape(tokens, -1)


def layer(h, w):
    a = normed(h)
    q, k = (turned(matmul(a, w[name]).reshape(h.shape[0], -1, HEAD), THETA) for name in ("wq", "wk"))
    h = h + matmul(seen_by(q, k, matmul(a, w["wv"]).reshape(h.shape[0], -1, HEAD)), w["wo"])
    b = normed(h)
    gate = jnp.dot(b, w["w_gate"], preferred_element_type=jnp.float32)
    up = jnp.dot(b, w["w_up"], preferred_element_type=jnp.float32)
    return h + matmul((jax.nn.silu(gate) * up).astype(jnp.bfloat16), w["w_down"])


def adamw(w, m, v, g):
    m = 0.9 * m + 0.1 * g
    v = 0.95 * v + 0.05 * g * g
    step = m * lax.rsqrt(v + 1e-8) + 0.1 * w
    return (w - 0.02 * step).astype(jnp.bfloat16), m, v


def clipped(gradients, sum_of_squares, count):
    factor = jnp.minimum(1.0, 0.5 * lax.rsqrt(sum_of_squares / count + 1e-30))
    return [g * factor for g in gradients]


def stack(weights, h):
    return lax.scan(lambda h, w: (layer(h, w), None), h, weights)[0]


def reference(x, dy, wq, wk, wv, wo, w_gate, w_up, w_down, m_wq, m_wk, m_wv, m_wo, m_w_gate, m_w_up, m_w_down, v_wq, v_wk, v_wv, v_wo, v_w_gate, v_w_up, v_w_down):
    weights = dict(zip(NAMES, (wq, wk, wv, wo, w_gate, w_up, w_down), strict=True))

    def take(so_far, sequence):
        h, by_y = sequence
        _, back = jax.vjp(stack, weights, h)
        by_weights, by_h = back(by_y)
        return jax.tree.map(lambda total, term: total + term.astype(jnp.float32), so_far, by_weights), by_h

    none_yet = {name: jnp.zeros(w.shape, jnp.float32) for name, w in weights.items()}
    by_weights, by_x = lax.scan(take, none_yet, (x, dy))
    gradients = [by_weights[name].astype(jnp.bfloat16).astype(jnp.float32) for name in NAMES]
    gradients = clipped(gradients, sum(jnp.sum(g * g) for g in gradients), sum(g.size for g in gradients))
    first = (m_wq, m_wk, m_wv, m_wo, m_w_gate, m_w_up, m_w_down)
    second = (v_wq, v_wk, v_wv, v_wo, v_w_gate, v_w_up, v_w_down)
    new = [adamw(weights[name].astype(jnp.float32), m, v, g) for name, m, v, g in zip(NAMES, first, second, gradients, strict=True)]
    return tuple(one[which] for which in range(3) for one in new)
```

```python
import functools

import jax
import jax.numpy as jnp
from jax import lax
from jax.experimental import pallas as pl
from jax.experimental.pallas import tpu as pltpu
from jax.sharding import PartitionSpec as P

HEAD = 128
THETA = 10000
NAMES = ("wq", "wk", "wv", "wo", "w_gate", "w_up", "w_down")
NEG = -1e30
HIDDEN = 2 * NEG
LOG2E = 1.4426950408889634
FORWARD = (512, 512)
BACKWARD = (512, 512)
MESH = pl.DeviceIdType.MESH
CORES = 2


def _dot(a, b, ca, cb):
    return lax.dot_general(a, b, (((ca,), (cb,)), ((), ())), preferred_element_type=jnp.float32)


def _gap(bk, bq):
    return lax.broadcasted_iota(jnp.int32, (bk, bq), 1) - lax.broadcasted_iota(jnp.int32, (bk, bq), 0)


def _attend(q_ref, k_ref, v_ref, o_ref, lse_ref, top_s, mix_s, *, scale, bk, wide):
    heads, bq, d = q_ref.shape
    iq = pl.program_id(0)
    e = scale * LOG2E
    pieces = [(i, at) for i in range(heads) for at in range(0, bq, wide)]
    top_s[...] = jnp.full_like(top_s, NEG)
    mix_s[...] = jnp.zeros_like(mix_s)
    ones = jnp.ones((8, bk), BF16)
    gap = _gap(bk, wide)

    def block(j, masked):
        here = pl.ds(pl.multiple_of(j * bk, bk), bk)
        scores = [_dot(k_ref[i, here, :], q_ref[i, at : at + wide, :], 1, 1) for i, at in pieces]
        weights, keeps = [], []
        for (i, at), s in zip(pieces, scores):
            if masked:
                s = jnp.where(gap >= j * bk - iq * bq - at, s, HIDDEN)
            old = top_s[i : i + 1, at : at + wide]
            top = jnp.maximum(old, s.max(axis=0, keepdims=True))
            top_s[i : i + 1, at : at + wide] = top
            weights.append(jnp.exp2((s - top) * e).astype(BF16))
            keeps.append(jnp.exp2((old - top) * e))
        for (i, at), p, keep in zip(pieces, weights, keeps):
            values = jnp.concatenate([v_ref[i, here, :].T, ones], axis=0)
            mix_s[i, :, at : at + wide] = mix_s[i, :, at : at + wide] * keep + _dot(values, p, 1, 0)

    whole = lax.div(iq * bq, bk)
    lax.fori_loop(0, whole, lambda j, _: block(j, False), None)
    lax.fori_loop(whole, lax.div((iq + 1) * bq + bk - 1, bk), lambda j, _: block(j, True), None)
    for i in range(heads):
        total = mix_s[i, d : d + 1, :]
        o_ref[i] = (mix_s[i, :d, :] * (1 / total)).T.astype(o_ref.dtype)
        lse_ref[i : i + 1, :] = top_s[i : i + 1, :] * scale + jnp.log(total)


def attend(q, k, v):
    heads, tokens, d = q.shape
    bq, bk = FORWARD
    spec = pl.BlockSpec((heads, bq, d), lambda i: (0, i, 0))
    return pl.pallas_call(
        functools.partial(_attend, scale=d**-0.5, bk=bk, wide=min(bq, 512)),
        grid=(tokens // bq,),
        in_specs=[spec] + [_whole((heads, tokens, d), 0, 0, 0)] * 2,
        out_specs=[spec, pl.BlockSpec((heads, bq), lambda i: (0, i))],
        out_shape=[jax.ShapeDtypeStruct(q.shape, BF16), jax.ShapeDtypeStruct((heads, tokens), F32)],
        scratch_shapes=[pltpu.VMEM((heads, bq), F32), pltpu.VMEM((heads, d + 8, bq), F32)],
        compiler_params=pltpu.CompilerParams(dimension_semantics=("arbitrary",), vmem_limit_bytes=ROOM),
        cost_estimate=pl.CostEstimate(flops=4 * heads * tokens * tokens * d, transcendentals=heads * tokens * tokens, bytes_accessed=8 * q.size),
    )(q, k, v)


def _attend_back(q_ref, k_ref, v_ref, do_ref, lse_ref, delta_ref, dq_ref, dk_ref, dv_ref, dq_s, dk_s, dv_s, *, scale, bk):
    heads, bq, d = q_ref.shape
    iq = pl.program_id(0)
    e = scale * LOG2E

    @pl.when(iq == 0)
    def _():
        dk_s[...] = jnp.zeros_like(dk_s)
        dv_s[...] = jnp.zeros_like(dv_s)

    dq_s[...] = jnp.zeros_like(dq_s)
    lses = [lse_ref[i : i + 1, :] * LOG2E for i in range(heads)]
    deltas = [delta_ref[i : i + 1, :] for i in range(heads)]
    gap = _gap(bk, bq)

    def block(j, masked):
        here = pl.ds(pl.multiple_of(j * bk, bk), bk)
        scores = [_dot(k_ref[i, here, :], q_ref[i], 1, 1) for i in range(heads)]
        dps = [_dot(v_ref[i, here, :], do_ref[i], 1, 1) for i in range(heads)]
        for i in range(heads):
            p = jnp.exp2(scores[i] * e - lses[i])
            if masked:
                p = jnp.where(gap >= j * bk - iq * bq, p, 0.0)
            ds = (p * (dps[i] - deltas[i])).astype(BF16)
            dv_s[i, here, :] += _dot(p.astype(BF16), do_ref[i], 1, 0)
            dk_s[i, here, :] += _dot(ds, q_ref[i], 1, 0)
            dq_s[i] += _dot(k_ref[i, here, :].T, ds, 1, 0)

    whole = lax.div(iq * bq, bk)
    lax.fori_loop(0, whole, lambda j, _: block(j, False), None)
    lax.fori_loop(whole, lax.div((iq + 1) * bq + bk - 1, bk), lambda j, _: block(j, True), None)
    for i in range(heads):
        dq_ref[i] = (dq_s[i] * scale).T.astype(BF16)

    @pl.when(iq == pl.num_programs(0) - 1)
    def _():
        dk_ref[...] = (dk_s[...] * scale).astype(BF16)
        dv_ref[...] = dv_s[...].astype(BF16)


def attend_back(q, k, v, do, lse, delta):
    heads, tokens, d = q.shape
    bq, bk = BACKWARD
    spec = pl.BlockSpec((heads, bq, d), lambda i: (0, i, 0))
    stats = pl.BlockSpec((heads, bq), lambda i: (0, i))
    every = _whole(q.shape, 0, 0, 0)
    return pl.pallas_call(
        functools.partial(_attend_back, scale=d**-0.5, bk=bk),
        grid=(tokens // bq,),
        in_specs=[spec, every, every, spec, stats, stats],
        out_specs=[spec, every, every],
        out_shape=[jax.ShapeDtypeStruct(q.shape, BF16)] * 3,
        scratch_shapes=[pltpu.VMEM((heads, d, bq), F32), pltpu.VMEM(q.shape, F32), pltpu.VMEM(q.shape, F32)],
        compiler_params=pltpu.CompilerParams(dimension_semantics=("arbitrary",), vmem_limit_bytes=ROOM),
        cost_estimate=pl.CostEstimate(flops=10 * heads * tokens * tokens * d, transcendentals=heads * tokens * tokens, bytes_accessed=14 * q.size),
    )(q, k, v, do, lse, delta)


F32, BF16 = jnp.float32, jnp.bfloat16
ROOM = 60 * 2**20
TOKENS = 512


def scaled(h):
    wide = h.astype(F32)
    return wide, lax.rsqrt(jnp.mean(wide * wide, -1, keepdims=True) + 1e-6)


def unscaled(wide, scale, by_out):
    dot = jnp.sum(by_out * wide, -1, keepdims=True)
    return by_out * scale - wide * (scale * scale * scale * dot * (1.0 / wide.shape[-1]))


def tables(tokens, theta):
    half = HEAD // 2
    angle = jnp.arange(tokens, dtype=F32)[:, None] * theta ** (-jnp.arange(half, dtype=F32) / half)
    cos, sin = jnp.cos(angle), jnp.sin(angle)
    return jnp.concatenate([cos, cos], -1), jnp.concatenate([-sin, sin], -1)


def heads_of(ref):
    return jnp.concatenate([ref[i] for i in range(ref.shape[0])], axis=1)


def piece(ref, at, rows):
    return ref[:, at : at + rows, :].reshape(ref.shape[0] * rows, ref.shape[2])


def _qkv(h_ref, w_ref, cos_ref, sin_ref, q_ref, k_ref, v_ref):
    wide, scale = scaled(h_ref[...])
    a = (wide * scale).astype(BF16)
    rows = w_ref.shape[1] // 3
    cos, sin = cos_ref[...], sin_ref[...]
    for i, out in enumerate((q_ref, k_ref, v_ref)):
        t = _dot(a, piece(w_ref, i * rows, rows), 1, 0).astype(BF16)
        for n in range(out.shape[0]):
            one = t[:, n * HEAD : (n + 1) * HEAD]
            if i < 2:
                one = one.astype(F32)
                one = (one * cos + pltpu.roll(one, HEAD // 2, 1) * sin).astype(BF16)
            out[n] = one


def _mlp(h_ref, o_ref, wo_ref, gate_ref, up_ref, down_ref, y_ref, prod_s):
    d = h_ref.shape[1]
    rows = d // gate_ref.shape[0]
    h = (h_ref[...].astype(F32) + _dot(heads_of(o_ref), piece(wo_ref, 0, wo_ref.shape[1]), 1, 0).astype(BF16).astype(F32)).astype(BF16)
    wide, scale = scaled(h)
    b = (wide * scale).astype(BF16)
    for c in range(prod_s.shape[1] // d):
        gate = _dot(b, piece(gate_ref, c * rows, rows), 1, 0)
        up = _dot(b, piece(up_ref, c * rows, rows), 1, 0)
        prod_s[:, c * d : (c + 1) * d] = (gate * jax.nn.sigmoid(gate) * up).astype(BF16)
    down = _dot(prod_s[...], piece(down_ref, 0, down_ref.shape[1]), 1, 0).astype(BF16)
    y_ref[...] = (wide + down.astype(F32)).astype(BF16)


def _mlp_back(h_ref, o_ref, by_y_ref, wo_ref, gate_ref, up_ref, down_ref, *rest, extra):
    extra_ref, rest = (rest[0], rest[1:]) if extra else (None, rest)
    by_h_ref, by_o_ref, delta_ref, grads_ref, gate_s, up_s, down_s, o_s = rest
    n, (tokens, d) = gate_ref.shape[0], h_ref.shape
    rows, deep = d // n, down_ref.shape[1]
    step = pl.program_id(0)

    @pl.when(step == 0)
    def _():
        for s in (gate_s, up_s, down_s, o_s):
            s[...] = jnp.zeros_like(s)

    o = heads_of(o_ref)
    wo = piece(wo_ref, 0, wo_ref.shape[1])
    h = (h_ref[...].astype(F32) + _dot(o, wo, 1, 0).astype(BF16).astype(F32)).astype(BF16)
    wide, scale = scaled(h)
    b = (wide * scale).astype(BF16)
    by_y = by_y_ref[...]
    b_t, by_y_t = b.T, by_y.T
    by_b = jnp.zeros((tokens, d), F32)
    for c in range(gate_s.shape[1] // d):
        here = slice(c * d, (c + 1) * d)
        w_gate, w_up = piece(gate_ref, c * rows, rows), piece(up_ref, c * rows, rows)
        owners = d // deep
        w_down = down_ref[c * owners : (c + 1) * owners].reshape(d, d)
        gate = _dot(b, w_gate, 1, 0)
        up = _dot(b, w_up, 1, 0)
        by_prod = _dot(by_y, w_down, 1, 1).astype(BF16).astype(F32)
        sig = jax.nn.sigmoid(gate)
        silu = gate * sig
        prod = (silu * up).astype(BF16)
        by_up = (by_prod * silu).astype(BF16)
        by_gate = (by_prod * up * (sig + silu * (1.0 - sig))).astype(BF16)
        by_b = by_b + _dot(by_gate, w_gate, 1, 1) + _dot(by_up, w_up, 1, 1)
        gate_s[:, here] += _dot(b_t, by_gate, 1, 0)
        up_s[:, here] += _dot(b_t, by_up, 1, 0)
        down_s[:, here] += _dot(by_y_t, prod, 1, 0)
    by_norm = unscaled(wide, scale, by_b.astype(BF16).astype(F32)).astype(BF16)
    by_h = (by_y.astype(F32) + by_norm.astype(F32)).astype(BF16)
    by_h_ref[...] = by_h
    o_s[...] += _dot(o.T, by_h, 1, 0)
    by_o = _dot(by_h, wo, 1, 1).astype(BF16)
    for i in range(by_o_ref.shape[0]):
        one = by_o[:, i * HEAD : (i + 1) * HEAD]
        by_o_ref[i] = one
        delta_ref[i : i + 1, :] = jnp.sum((one.astype(F32) * o_ref[i].astype(F32)).T, axis=0, keepdims=True)

    @pl.when(step == pl.num_programs(0) - 1)
    def _():
        chunks = gate_s.shape[1] // d
        at = chunks * rows
        for c in range(chunks):
            here = slice(c * d, (c + 1) * d)
            grads_ref[:, c * rows : (c + 1) * rows, :] = gate_s[:, here].astype(BF16).reshape(n, rows, d)
            grads_ref[:, at + c * rows : at + (c + 1) * rows, :] = up_s[:, here].astype(BF16).reshape(n, rows, d)
            owners = d // deep
            grads_ref[c * owners : (c + 1) * owners, 2 * at : 2 * at + deep, :] = down_s[:, here].T.astype(BF16).reshape(owners, deep, d)
        at = 2 * at + deep
        own = o_s.shape[0] // n
        grads_ref[:, at : at + own, :] = o_s[...].astype(BF16).reshape(n, own, d)
        if extra:
            grads_ref[:, at + own :, :] = extra_ref[...]


def _qkv_back(h_ref, by_q_ref, by_k_ref, by_v_ref, cos_ref, sin_ref, *rest, last):
    if last:
        grads_ref, total_s = rest
    else:
        w_ref, by_h_ref, out_ref, grads_ref, total_s = rest
    d = h_ref.shape[1]
    n, rows = grads_ref.shape[0], grads_ref.shape[1] // 3
    step = pl.program_id(0)

    @pl.when(step == 0)
    def _():
        total_s[...] = jnp.zeros_like(total_s)

    wide, scale = scaled(h_ref[...])
    a_t = (wide * scale).astype(BF16).T
    cos, sin = cos_ref[...], sin_ref[...]
    by_a = None
    for i, ref in enumerate((by_q_ref, by_k_ref, by_v_ref)):
        if i < 2:
            parts = []
            for m in range(ref.shape[0]):
                one = ref[m].astype(F32)
                parts.append((one * cos - pltpu.roll(one, HEAD // 2, 1) * sin).astype(BF16))
            x = jnp.concatenate(parts, axis=1)
        else:
            x = heads_of(ref)
        total_s[i] += _dot(a_t, x, 1, 0)
        if not last:
            term = _dot(x, piece(w_ref, i * rows, rows), 1, 1)
            by_a = term if by_a is None else by_a + term
    if not last:
        by_norm = unscaled(wide, scale, by_a.astype(BF16).astype(F32)).astype(BF16)
        out_ref[...] = (by_h_ref[...].astype(F32) + by_norm.astype(F32)).astype(BF16)

    @pl.when(step == pl.num_programs(0) - 1)
    def _():
        for i in range(3):
            grads_ref[:, i * rows : (i + 1) * rows, :] = total_s[i].astype(BF16).reshape(n, rows, d)


def _whole(shape, *at):
    return pl.BlockSpec(shape, lambda i: at, pipeline_mode=pl.Buffered(1))


def _rows(d):
    return pl.BlockSpec((TOKENS, d), lambda i: (i, 0))


def _heads(heads):
    return pl.BlockSpec((heads, TOKENS, HEAD), lambda i: (0, i, 0))


def _call(body, tokens, in_specs, out_specs, out_shape, scratch, flops, args, exps=0):
    moved = sum(a.size * a.dtype.itemsize for a in (*args, *out_shape))
    return pl.pallas_call(
        body,
        grid=(tokens // TOKENS,),
        in_specs=in_specs,
        out_specs=out_specs,
        out_shape=out_shape,
        scratch_shapes=scratch,
        compiler_params=pltpu.CompilerParams(dimension_semantics=("arbitrary",), vmem_limit_bytes=ROOM),
        cost_estimate=pl.CostEstimate(flops=flops, transcendentals=exps, bytes_accessed=moved),
    )(*args)


def qkv(h, w, number, turn):
    (tokens, d), n = h.shape, w.shape[0]
    rows, heads = d // n, d // HEAD
    one = jax.ShapeDtypeStruct((heads, tokens, HEAD), BF16)
    return _call(_qkv, tokens, [_rows(d), _whole((n, 3 * rows, d), 0, number, 0), _rows(HEAD), _rows(HEAD)], [_heads(heads)] * 3, [one] * 3, [],
                 6 * tokens * d * d, (h, w, *turn))


def _matrices(w, d, ff):
    n = w.shape[0]
    rows, deep = d // n, ff // n
    return [_whole((n, rows, d), 0, 3 * deep // rows, 0)] + [_whole((n, deep, d), 0, i, 0) for i in range(3)]


def mlp(h, o, w, ff):
    (tokens, d), heads = h.shape, o.shape[0]
    return _call(_mlp, tokens, [_rows(d), _heads(heads)] + _matrices(w, d, ff), [_rows(d)], [jax.ShapeDtypeStruct((tokens, d), BF16)],
                 [pltpu.VMEM((TOKENS, ff), BF16)], 2 * tokens * d * (d + 3 * ff), (h, o, w, w, w, w), tokens * ff)[0]


def mlp_back(h, o, by_y, w, ff, extra):
    (tokens, d), heads, n = h.shape, o.shape[0], w.shape[0]
    size = (3 * ff + d) // n + (0 if extra is None else extra.shape[1])
    more = [] if extra is None else [extra]
    return _call(functools.partial(_mlp_back, extra=extra is not None), tokens,
                 [_rows(d), _heads(heads), _rows(d)] + _matrices(w, d, ff) + [_whole(e.shape, 0, 0, 0) for e in more],
                 [_rows(d), _heads(heads), pl.BlockSpec((heads, TOKENS), lambda i: (0, i)), _whole((n, size, d), 0, 0, 0)],
                 [jax.ShapeDtypeStruct((tokens, d), BF16), jax.ShapeDtypeStruct((heads, tokens, HEAD), BF16),
                  jax.ShapeDtypeStruct((heads, tokens), F32), jax.ShapeDtypeStruct((n, size, d), BF16)],
                 [pltpu.VMEM((d, ff), F32)] * 3 + [pltpu.VMEM((heads * HEAD, d), F32)],
                 2 * tokens * d * (3 * d + 8 * ff), (h, o, by_y, w, w, w, w, *more), tokens * ff)


def qkv_back(h, by_q, by_k, by_v, turn, w, number, by_h):
    (tokens, d), heads, n = h.shape, by_q.shape[0], w.shape[0]
    rows = d // n
    last = by_h is None
    specs = [_rows(d)] + [_heads(heads)] * 3 + [_rows(HEAD)] * 2
    args = [h, by_q, by_k, by_v, *turn]
    outs, shapes = [_whole((n, 3 * rows, d), 0, 0, 0)], [jax.ShapeDtypeStruct((n, 3 * rows, d), BF16)]
    if not last:
        specs += [_whole((n, 3 * rows, d), 0, number, 0), _rows(d)]
        args += [w, by_h]
        outs, shapes = [_rows(d)] + outs, [jax.ShapeDtypeStruct((tokens, d), BF16)] + shapes
    got = _call(functools.partial(_qkv_back, last=last), tokens, specs, outs, shapes, [pltpu.VMEM((3, d, heads * HEAD), F32)],
                (6 if last else 12) * tokens * d * d, args)
    return (None, got[0]) if last else got


def _place(n):
    me = lax.axis_index("dp")
    return lax.div(me, CORES), lax.rem(me, CORES), n // CORES


def _greet(others):
    barrier = pltpu.get_barrier_semaphore()
    for other in others:
        pl.semaphore_signal(barrier, inc=1, device_id={"dp": other}, device_id_type=MESH)
    pl.semaphore_wait(barrier, len(others))


def _send(src, dst, sems, i, to):
    copy = pltpu.make_async_remote_copy(src_ref=src, dst_ref=dst, send_sem=sems[0].at[i], recv_sem=sems[1].at[i], device_id={"dp": to},
                                        device_id_type=MESH)
    copy.start()
    return copy


def _gather(x_ref, out_ref, right_send, right_recv, left_send, left_recv, pair_send, pair_recv, own_sem):
    n = out_ref.shape[0]
    chip, core, chips = _place(n)
    at = lambda c, k: lax.rem(c + 2 * chips, chips) * CORES + k
    me, partner = at(chip, core), at(chip, 1 - core)
    right, left = at(chip + 1, core), at(chip - 1, core)
    _greet((left, right, partner))
    own = pltpu.make_async_copy(x_ref, out_ref.at[me], own_sem)
    own.start()
    ways = ((right, (right_send, right_recv), chips // 2, -1), (left, (left_send, left_recv), (chips - 1) // 2, 1))
    moving = [[_send(x_ref, out_ref.at[me], sems, 0, to)] for to, sems, _, _ in ways]
    pairs = [_send(x_ref, out_ref.at[me], (pair_send, pair_recv), 0, partner)]
    for step in range(1, chips // 2 + 1):
        for (to, sems, last, sign), copies in zip(ways, moving):
            if step <= last:
                came = out_ref.at[at(chip + sign * step, core)]
                copies[step - 1].wait_recv()
                if step < last:
                    copies.append(_send(came, came, sems, step, to))
                pairs.append(_send(came, came, (pair_send, pair_recv), len(pairs), partner))
    for copy in pairs:
        copy.wait()
    for copies in moving:
        for copy in copies:
            copy.wait_send()
    own.wait()


def gather(x, n):
    chips = n // CORES
    dma = pltpu.SemaphoreType.DMA
    near, far = max((chips - 1) // 2, 1), chips // 2
    vmem = pl.BlockSpec(memory_space=pltpu.VMEM)
    return pl.pallas_call(
        _gather,
        in_specs=[vmem],
        out_specs=vmem,
        out_shape=jax.ShapeDtypeStruct((n, *x.shape), x.dtype),
        scratch_shapes=[dma((far,)), dma((far,)), dma((near,)), dma((near,)), dma((chips,)), dma((chips,)), dma],
        compiler_params=pltpu.CompilerParams(collective_id=1, has_side_effects=True, vmem_limit_bytes=ROOM),
        cost_estimate=pl.CostEstimate(flops=2 * 10**9, transcendentals=0, bytes_accessed=n * x.size * 2),
    )(x)


def _scatter(x_ref, out_ref, pair_s, right_s, left_s, right_in, left_in, pair_send, pair_recv, right_send, right_recv, left_send, left_recv):
    n = x_ref.shape[0]
    chip, core, chips = _place(n)
    at = lambda c, k: lax.rem(c + 2 * chips, chips) * CORES + k
    partner, right, left = at(chip, 1 - core), at(chip + 1, core), at(chip - 1, core)
    far, near = chips // 2, (chips - 1) // 2
    _greet((left, right, partner))
    order = []
    for step in range(far):
        order.append(far - step)
        if step < near:
            order.append(step - near)
    order.append(0)
    pairs = [_send(x_ref.at[at(chip + away, 1 - core)], pair_s.at[i], (pair_send, pair_recv), i, partner) for i, away in enumerate(order)]

    def term(away):
        i = order.index(away)
        pairs[i].wait_recv()
        return x_ref[at(chip + away, core)].astype(F32) + pair_s[i].astype(F32)

    rights, lefts = [], []
    for step in range(far):
        total = term(far - step)
        if step:
            rights[-1].wait_recv()
            total = total + right_in[step - 1].astype(F32)
        right_s[step] = total.astype(BF16)
        rights.append(_send(right_s.at[step], right_in.at[step], (right_send, right_recv), step, right))
        if step < near:
            total = term(step - near)
            if step:
                lefts[-1].wait_recv()
                total = total + left_in[step - 1].astype(F32)
            left_s[step] = total.astype(BF16)
            lefts.append(_send(left_s.at[step], left_in.at[step], (left_send, left_recv), step, left))
    total = term(0)
    if lefts:
        lefts[-1].wait_recv()
        total = total + left_in[near - 1].astype(F32)
    rights[-1].wait_recv()
    total = total + right_in[far - 1].astype(F32)
    out_ref[...] = total.astype(BF16)
    for copy in (*pairs, *rights, *lefts):
        copy.wait_send()


def scatter(x):
    n, *block = x.shape
    chips = n // CORES
    far, near = chips // 2, max((chips - 1) // 2, 1)
    dma = pltpu.SemaphoreType.DMA
    vmem = pl.BlockSpec(memory_space=pltpu.VMEM)
    room = lambda count: pltpu.VMEM((count, *block), BF16)
    return pl.pallas_call(
        _scatter,
        in_specs=[vmem],
        out_specs=vmem,
        out_shape=jax.ShapeDtypeStruct(tuple(block), BF16),
        scratch_shapes=[room(chips), room(far), room(near), room(far), room(near)] + [dma((chips,))] * 2 + [dma((far,))] * 2 + [dma((near,))] * 2,
        compiler_params=pltpu.CompilerParams(collective_id=2, has_side_effects=True, vmem_limit_bytes=ROOM),
        cost_estimate=pl.CostEstimate(flops=10**9, transcendentals=0, bytes_accessed=2 * x.size),
    )(x)


def _squares(*refs, n):
    *block_refs, out_ref, mine, sums, send_sem, recv_sem = refs
    chip, core, chips = _place(n)
    me = lax.axis_index("dp")
    others = [lax.rem(me + i, n) for i in range(1, n)]
    total = jnp.zeros((8, 128), F32)
    for ref in block_refs:
        x = ref[...].astype(F32)
        x = jnp.sum((x * x).reshape(-1, 8, x.shape[1]), axis=0)
        for at in range(0, x.shape[1], 128):
            total = total + x[:, at : at + 128]
    mine[...] = total
    _greet(others)
    copies = [_send(mine, sums.at[i], (send_sem, recv_sem), i, other) for i, other in enumerate(others)]
    for i, copy in enumerate(copies):
        copy.wait_recv()
        total = total + sums[i]
    for copy in copies:
        copy.wait_send()
    out_ref[...] = total


def squares(blocks, n):
    vmem = pl.BlockSpec(memory_space=pltpu.VMEM)
    dma = pltpu.SemaphoreType.DMA
    return pl.pallas_call(
        functools.partial(_squares, n=n),
        in_specs=[vmem] * len(blocks),
        out_specs=vmem,
        out_shape=jax.ShapeDtypeStruct((8, 128), F32),
        scratch_shapes=[pltpu.VMEM((8, 128), F32), pltpu.VMEM((n - 1, 8, 128), F32), dma((n - 1,)), dma((n - 1,))],
        compiler_params=pltpu.CompilerParams(collective_id=3, has_side_effects=True),
        cost_estimate=pl.CostEstimate(flops=10**8, transcendentals=0, bytes_accessed=2 * sum(b.size for b in blocks)),
    )(*blocks).sum()


def adamw(w, m, v, g):
    m = 0.9 * m + 0.1 * g
    v = 0.95 * v + 0.05 * g * g
    step = m * lax.rsqrt(v + 1e-8) + 0.1 * w
    return (w - 0.02 * step).astype(BF16), m, v


def factor_of(sum_of_squares, count):
    return jnp.minimum(1.0, 0.5 * lax.rsqrt(sum_of_squares / count + 1e-30))


def cut(t, d):
    rows = t.shape[0]
    return t.reshape(rows, -1, d).transpose(1, 0, 2).reshape(-1, d)


def joined(t, rows):
    return t.reshape(-1, rows, t.shape[1]).transpose(1, 0, 2).reshape(rows, -1)


def solution(mesh):
    def step(x, dy, *arrays):
        weights, m, v = (arrays[i : i + 7] for i in (0, 7, 14))
        layers, rows, d = weights[0].shape
        deep = weights[6].shape[1]
        n = mesh.shape["dp"]
        ff = deep * n
        wide = ff // d * rows
        turn = tables(x.shape[1], THETA)
        first = gather(jnp.concatenate([w[i] for i in range(layers) for w in weights[:3]]), n)
        rest = [lax.all_gather(jnp.concatenate([cut(weights[j][i], d) for j in (4, 5, 6, 3)]), "dp", axis=0, tiled=False) for i in range(layers)]
        h, kept = x[0], []
        for i in range(layers):
            q, k, val = qkv(h, first, i, turn)
            o, lse = attend(q, k, val)
            kept.append((h, q, k, val, o, lse))
            if i < layers - 1:
                h = mlp(h, o, rest[i], ff)
        by_h, extra = dy[0], None
        blocks, sums = {}, []
        for i in reversed(range(layers)):
            h, q, k, val, o, lse = kept[i]
            by_mid, by_o, delta, grads = mlp_back(h, o, by_h, rest[i], ff, extra)
            if sums:
                by_o, sums[-1] = lax.optimization_barrier((by_o, sums[-1]))
            sums.append(lax.psum_scatter(grads, "dp", scatter_dimension=0, tiled=False))
            by_q, by_k, by_v = attend_back(q, k, val, by_o, lse, delta)
            by_h, extra = qkv_back(h, by_q, by_k, by_v, turn, first, i, by_mid if i else None)
        sums.append(scatter(extra))
        for i, got in zip(reversed(range(layers)), sums):
            for name, at, size in (("w_gate", 0, wide), ("w_up", wide, wide), ("w_down", 2 * wide, deep), ("wo", 2 * wide + deep, rows)):
                blocks[name, i] = got[at : at + size]
        for i, got in zip(reversed(range(layers)), sums[1:]):
            at = got.shape[0] - 3 * rows
            for j, name in enumerate(("wq", "wk", "wv")):
                blocks[name, i] = got[at + j * rows : at + (j + 1) * rows]
        factor = factor_of(squares(sums, n), n * sum(w.size for w in weights))
        new = []
        for name, w, m_, v_ in zip(NAMES, weights, m, v, strict=True):
            g = jnp.stack([joined(blocks[name, i], w.shape[1]) for i in range(layers)]).astype(F32) * factor
            new.append(adamw(w.astype(F32), m_, v_, g))
        return tuple(one[which] for which in range(3) for one in new)

    states, cut_ = P(("rep", "dp"), None, None), P(None, "dp", None)
    return jax.shard_map(
        step,
        mesh=mesh,
        in_specs=(states, states) + (cut_,) * 21,
        out_specs=(P("rep", "dp", None),) * 21,
        check_vma=False,
    )
```

```python
import functools

import jax
import jax.numpy as jnp
import numpy as np
from jax import lax
from jax.experimental import pallas as pl
from jax.experimental.pallas import tpu as pltpu
from jax.sharding import PartitionSpec as P

HEAD = 128
THETA = 10000
NAMES = ("wq", "wk", "wv", "wo", "w_gate", "w_up", "w_down")
NEG = -1e30
HIDDEN = 2 * NEG
LOG2E = 1.4426950408889634
FORWARD = (512, 512)
BACKWARD = (512, 512)
MESH = pl.DeviceIdType.MESH
CORES = 2


def _dot(a, b, ca, cb):
    return lax.dot_general(a, b, (((ca,), (cb,)), ((), ())), preferred_element_type=jnp.float32)


def _gap(bk, bq):
    return lax.broadcasted_iota(jnp.int32, (bk, bq), 1) - lax.broadcasted_iota(jnp.int32, (bk, bq), 0)


def _attend(q_ref, k_ref, v_ref, o_ref, lse_ref, top_s, mix_s, *, scale, bk, wide):
    heads, bq, d = q_ref.shape
    iq = pl.program_id(0)
    e = scale * LOG2E
    pieces = [(i, at) for i in range(heads) for at in range(0, bq, wide)]
    top_s[...] = jnp.full_like(top_s, NEG)
    mix_s[...] = jnp.zeros_like(mix_s)
    ones = jnp.ones((8, bk), BF16)
    gap = _gap(bk, wide)

    def block(j, masked):
        here = pl.ds(pl.multiple_of(j * bk, bk), bk)
        scores = [_dot(k_ref[i, here, :], q_ref[i, at : at + wide, :], 1, 1) for i, at in pieces]
        weights, keeps = [], []
        for (i, at), s in zip(pieces, scores):
            if masked:
                s = jnp.where(gap >= j * bk - iq * bq - at, s, HIDDEN)
            old = top_s[i : i + 1, at : at + wide]
            top = jnp.maximum(old, s.max(axis=0, keepdims=True))
            top_s[i : i + 1, at : at + wide] = top
            weights.append(jnp.exp2((s - top) * e).astype(BF16))
            keeps.append(jnp.exp2((old - top) * e))
        for (i, at), p, keep in zip(pieces, weights, keeps):
            values = jnp.concatenate([v_ref[i, here, :].T, ones], axis=0)
            mix_s[i, :, at : at + wide] = mix_s[i, :, at : at + wide] * keep + _dot(values, p, 1, 0)

    whole = lax.div(iq * bq, bk)
    lax.fori_loop(0, whole, lambda j, _: block(j, False), None)
    lax.fori_loop(whole, lax.div((iq + 1) * bq + bk - 1, bk), lambda j, _: block(j, True), None)
    for i in range(heads):
        total = mix_s[i, d : d + 1, :]
        o_ref[i] = (mix_s[i, :d, :] * (1 / total)).T.astype(o_ref.dtype)
        lse_ref[i : i + 1, :] = top_s[i : i + 1, :] * scale + jnp.log(total)


def attend(q, k, v):
    heads, tokens, d = q.shape
    bq, bk = FORWARD
    spec = pl.BlockSpec((heads, bq, d), lambda i: (0, i, 0))
    return pl.pallas_call(
        functools.partial(_attend, scale=d**-0.5, bk=bk, wide=min(bq, 512)),
        grid=(tokens // bq,),
        in_specs=[spec] + [_whole((heads, tokens, d), 0, 0, 0)] * 2,
        out_specs=[spec, pl.BlockSpec((heads, bq), lambda i: (0, i))],
        out_shape=[jax.ShapeDtypeStruct(q.shape, BF16), jax.ShapeDtypeStruct((heads, tokens), F32)],
        scratch_shapes=[pltpu.VMEM((heads, bq), F32), pltpu.VMEM((heads, d + 8, bq), F32)],
        compiler_params=pltpu.CompilerParams(dimension_semantics=("arbitrary",), vmem_limit_bytes=ROOM),
        cost_estimate=pl.CostEstimate(flops=4 * heads * tokens * tokens * d, transcendentals=heads * tokens * tokens, bytes_accessed=8 * q.size),
    )(q, k, v)


def _attend_back(q_ref, k_ref, v_ref, do_ref, lse_ref, delta_ref, dq_ref, dk_ref, dv_ref, dq_s, dk_s, dv_s, *, scale, bk):
    heads, bq, d = q_ref.shape
    iq = pl.program_id(0)
    e = scale * LOG2E

    @pl.when(iq == 0)
    def _():
        dk_s[...] = jnp.zeros_like(dk_s)
        dv_s[...] = jnp.zeros_like(dv_s)

    dq_s[...] = jnp.zeros_like(dq_s)
    lses = [lse_ref[i : i + 1, :] * LOG2E for i in range(heads)]
    deltas = [delta_ref[i : i + 1, :] for i in range(heads)]
    gap = _gap(bk, bq)

    def block(j, masked):
        here = pl.ds(pl.multiple_of(j * bk, bk), bk)
        scores = [_dot(k_ref[i, here, :], q_ref[i], 1, 1) for i in range(heads)]
        dps = [_dot(v_ref[i, here, :], do_ref[i], 1, 1) for i in range(heads)]
        for i in range(heads):
            p = jnp.exp2(scores[i] * e - lses[i])
            if masked:
                p = jnp.where(gap >= j * bk - iq * bq, p, 0.0)
            ds = (p * (dps[i] - deltas[i])).astype(BF16)
            dv_s[i, here, :] += _dot(p.astype(BF16), do_ref[i], 1, 0)
            dk_s[i, here, :] += _dot(ds, q_ref[i], 1, 0)
            dq_s[i] += _dot(k_ref[i, here, :].T, ds, 1, 0)

    whole = lax.div(iq * bq, bk)
    lax.fori_loop(0, whole, lambda j, _: block(j, False), None)
    lax.fori_loop(whole, lax.div((iq + 1) * bq + bk - 1, bk), lambda j, _: block(j, True), None)
    for i in range(heads):
        dq_ref[i] = (dq_s[i] * scale).T.astype(BF16)

    @pl.when(iq == pl.num_programs(0) - 1)
    def _():
        dk_ref[...] = (dk_s[...] * scale).astype(BF16)
        dv_ref[...] = dv_s[...].astype(BF16)


def attend_back(q, k, v, do, lse, delta):
    heads, tokens, d = q.shape
    bq, bk = BACKWARD
    spec = pl.BlockSpec((heads, bq, d), lambda i: (0, i, 0))
    stats = pl.BlockSpec((heads, bq), lambda i: (0, i))
    every = _whole(q.shape, 0, 0, 0)
    return pl.pallas_call(
        functools.partial(_attend_back, scale=d**-0.5, bk=bk),
        grid=(tokens // bq,),
        in_specs=[spec, every, every, spec, stats, stats],
        out_specs=[spec, every, every],
        out_shape=[jax.ShapeDtypeStruct(q.shape, BF16)] * 3,
        scratch_shapes=[pltpu.VMEM((heads, d, bq), F32), pltpu.VMEM(q.shape, F32), pltpu.VMEM(q.shape, F32)],
        compiler_params=pltpu.CompilerParams(dimension_semantics=("arbitrary",), vmem_limit_bytes=ROOM),
        cost_estimate=pl.CostEstimate(flops=10 * heads * tokens * tokens * d, transcendentals=heads * tokens * tokens, bytes_accessed=14 * q.size),
    )(q, k, v, do, lse, delta)


F32, BF16 = jnp.float32, jnp.bfloat16
ROOM = 60 * 2**20
TOKENS = 1024


def scaled(h):
    wide = h.astype(F32)
    return wide, lax.rsqrt(jnp.mean(wide * wide, -1, keepdims=True) + 1e-6)


def unscaled(wide, scale, by_out):
    dot = jnp.sum(by_out * wide, -1, keepdims=True)
    return by_out * scale - wide * (scale * scale * scale * dot * (1.0 / wide.shape[-1]))


def tables(tokens, theta):
    half = HEAD // 2
    angle = np.arange(tokens, dtype=np.float32)[:, None] * (theta ** (-np.arange(half) / half)).astype(np.float32)
    cos, sin = np.cos(angle.astype(np.float64)), np.sin(angle.astype(np.float64))
    return jnp.asarray(np.concatenate([cos, cos], -1), F32), jnp.asarray(np.concatenate([-sin, sin], -1), F32)


def heads_of(ref):
    return jnp.concatenate([ref[i] for i in range(ref.shape[0])], axis=1)


def piece(ref, at, rows):
    return ref[:, at : at + rows, :].reshape(ref.shape[0] * rows, ref.shape[2])


def _qkv(h_ref, w_ref, cos_ref, sin_ref, q_ref, k_ref, v_ref):
    wide, scale = scaled(h_ref[...])
    a = (wide * scale).astype(BF16)
    rows = w_ref.shape[1] // 3
    cos, sin = cos_ref[...], sin_ref[...]
    for i, out in enumerate((q_ref, k_ref, v_ref)):
        t = _dot(a, piece(w_ref, i * rows, rows), 1, 0).astype(BF16)
        for n in range(out.shape[0]):
            one = t[:, n * HEAD : (n + 1) * HEAD]
            if i < 2:
                one = one.astype(F32)
                one = (one * cos + pltpu.roll(one, HEAD // 2, 1) * sin).astype(BF16)
            out[n] = one


def _mlp(h_ref, o_ref, wo_ref, gate_ref, up_ref, down_ref, y_ref, prod_s):
    d = h_ref.shape[1]
    rows = d // gate_ref.shape[0]
    h = (h_ref[...].astype(F32) + _dot(heads_of(o_ref), piece(wo_ref, 0, wo_ref.shape[1]), 1, 0).astype(BF16).astype(F32)).astype(BF16)
    wide, scale = scaled(h)
    b = (wide * scale).astype(BF16)
    for c in range(prod_s.shape[1] // d):
        gate = _dot(b, piece(gate_ref, c * rows, rows), 1, 0)
        up = _dot(b, piece(up_ref, c * rows, rows), 1, 0)
        prod_s[:, c * d : (c + 1) * d] = (gate * jax.nn.sigmoid(gate) * up).astype(BF16)
    down = _dot(prod_s[...], piece(down_ref, 0, down_ref.shape[1]), 1, 0).astype(BF16)
    y_ref[...] = (wide + down.astype(F32)).astype(BF16)


def _mlp_back(h_ref, o_ref, by_y_ref, wo_ref, gate_ref, up_ref, down_ref, *rest, extra):
    extra_ref, rest = (rest[0], rest[1:]) if extra else (None, rest)
    by_h_ref, by_o_ref, delta_ref, grads_ref, gate_s, up_s, down_s, o_s = rest
    n, (tokens, d) = gate_ref.shape[0], h_ref.shape
    rows, deep = d // n, down_ref.shape[1]
    step = pl.program_id(0)

    @pl.when(step == 0)
    def _():
        for s in (gate_s, up_s, down_s, o_s):
            s[...] = jnp.zeros_like(s)

    o = heads_of(o_ref)
    wo = piece(wo_ref, 0, wo_ref.shape[1])
    h = (h_ref[...].astype(F32) + _dot(o, wo, 1, 0).astype(BF16).astype(F32)).astype(BF16)
    wide, scale = scaled(h)
    b = (wide * scale).astype(BF16)
    by_y = by_y_ref[...]
    b_t, by_y_t = b.T, by_y.T
    by_b = jnp.zeros((tokens, d), F32)
    for c in range(gate_s.shape[1] // d):
        here = slice(c * d, (c + 1) * d)
        w_gate, w_up = piece(gate_ref, c * rows, rows), piece(up_ref, c * rows, rows)
        owners = d // deep
        w_down = down_ref[c * owners : (c + 1) * owners].reshape(d, d)
        gate = _dot(b, w_gate, 1, 0)
        up = _dot(b, w_up, 1, 0)
        by_prod = _dot(by_y, w_down, 1, 1).astype(BF16).astype(F32)
        sig = jax.nn.sigmoid(gate)
        silu = gate * sig
        prod = (silu * up).astype(BF16)
        by_up = (by_prod * silu).astype(BF16)
        by_gate = (by_prod * up * (sig + silu * (1.0 - sig))).astype(BF16)
        by_b = by_b + _dot(by_gate, w_gate, 1, 1) + _dot(by_up, w_up, 1, 1)
        gate_s[:, here] += _dot(b_t, by_gate, 1, 0)
        up_s[:, here] += _dot(b_t, by_up, 1, 0)
        down_s[:, here] += _dot(by_y_t, prod, 1, 0)
    by_norm = unscaled(wide, scale, by_b.astype(BF16).astype(F32)).astype(BF16)
    by_h = (by_y.astype(F32) + by_norm.astype(F32)).astype(BF16)
    by_h_ref[...] = by_h
    o_s[...] += _dot(o.T, by_h, 1, 0)
    by_o = _dot(by_h, wo, 1, 1).astype(BF16)
    for i in range(by_o_ref.shape[0]):
        one = by_o[:, i * HEAD : (i + 1) * HEAD]
        by_o_ref[i] = one
        delta_ref[i : i + 1, :] = jnp.sum((one.astype(F32) * o_ref[i].astype(F32)).T, axis=0, keepdims=True)

    @pl.when(step == pl.num_programs(0) - 1)
    def _():
        chunks = gate_s.shape[1] // d
        at = chunks * rows
        for c in range(chunks):
            here = slice(c * d, (c + 1) * d)
            grads_ref[:, c * rows : (c + 1) * rows, :] = gate_s[:, here].astype(BF16).reshape(n, rows, d)
            grads_ref[:, at + c * rows : at + (c + 1) * rows, :] = up_s[:, here].astype(BF16).reshape(n, rows, d)
            owners = d // deep
            grads_ref[c * owners : (c + 1) * owners, 2 * at : 2 * at + deep, :] = down_s[:, here].T.astype(BF16).reshape(owners, deep, d)
        at = 2 * at + deep
        own = o_s.shape[0] // n
        grads_ref[:, at : at + own, :] = o_s[...].astype(BF16).reshape(n, own, d)
        if extra:
            grads_ref[:, at + own :, :] = extra_ref[...]


def _qkv_back(h_ref, by_q_ref, by_k_ref, by_v_ref, cos_ref, sin_ref, *rest, last):
    if last:
        grads_ref, total_s = rest
    else:
        w_ref, by_h_ref, out_ref, grads_ref, total_s = rest
    d = h_ref.shape[1]
    n, rows = grads_ref.shape[0], grads_ref.shape[1] // 3
    step = pl.program_id(0)

    @pl.when(step == 0)
    def _():
        total_s[...] = jnp.zeros_like(total_s)

    wide, scale = scaled(h_ref[...])
    a_t = (wide * scale).astype(BF16).T
    cos, sin = cos_ref[...], sin_ref[...]
    by_a = None
    for i, ref in enumerate((by_q_ref, by_k_ref, by_v_ref)):
        if i < 2:
            parts = []
            for m in range(ref.shape[0]):
                one = ref[m].astype(F32)
                parts.append((one * cos - pltpu.roll(one, HEAD // 2, 1) * sin).astype(BF16))
            x = jnp.concatenate(parts, axis=1)
        else:
            x = heads_of(ref)
        total_s[i] += _dot(a_t, x, 1, 0)
        if not last:
            term = _dot(x, piece(w_ref, i * rows, rows), 1, 1)
            by_a = term if by_a is None else by_a + term
    if not last:
        by_norm = unscaled(wide, scale, by_a.astype(BF16).astype(F32)).astype(BF16)
        out_ref[...] = (by_h_ref[...].astype(F32) + by_norm.astype(F32)).astype(BF16)

    @pl.when(step == pl.num_programs(0) - 1)
    def _():
        for i in range(3):
            grads_ref[:, i * rows : (i + 1) * rows, :] = total_s[i].astype(BF16).reshape(n, rows, d)


def _whole(shape, *at):
    return pl.BlockSpec(shape, lambda i: at, pipeline_mode=pl.Buffered(1))


def _rows(d):
    return pl.BlockSpec((TOKENS, d), lambda i: (i, 0))


def _heads(heads):
    return pl.BlockSpec((heads, TOKENS, HEAD), lambda i: (0, i, 0))


def _call(body, tokens, in_specs, out_specs, out_shape, scratch, flops, args, exps=0):
    moved = sum(a.size * a.dtype.itemsize for a in (*args, *out_shape))
    return pl.pallas_call(
        body,
        grid=(tokens // TOKENS,),
        in_specs=in_specs,
        out_specs=out_specs,
        out_shape=out_shape,
        scratch_shapes=scratch,
        compiler_params=pltpu.CompilerParams(dimension_semantics=("arbitrary",), vmem_limit_bytes=ROOM),
        cost_estimate=pl.CostEstimate(flops=flops, transcendentals=exps, bytes_accessed=moved),
    )(*args)


def qkv(h, w, number, turn):
    (tokens, d), n = h.shape, w.shape[0]
    rows, heads = d // n, d // HEAD
    one = jax.ShapeDtypeStruct((heads, tokens, HEAD), BF16)
    return _call(_qkv, tokens, [_rows(d), _whole((n, 3 * rows, d), 0, number, 0), _rows(HEAD), _rows(HEAD)], [_heads(heads)] * 3, [one] * 3, [],
                 6 * tokens * d * d, (h, w, *turn))


def _matrices(w, d, ff):
    n = w.shape[0]
    rows, deep = d // n, ff // n
    return [_whole((n, rows, d), 0, w.shape[1] // rows - 1, 0)] + [_whole((n, deep, d), 0, i, 0) for i in range(3)]


def mlp(h, o, w, ff):
    (tokens, d), heads = h.shape, o.shape[0]
    return _call(_mlp, tokens, [_rows(d), _heads(heads)] + _matrices(w, d, ff), [_rows(d)], [jax.ShapeDtypeStruct((tokens, d), BF16)],
                 [pltpu.VMEM((TOKENS, ff), BF16)], 2 * tokens * d * (d + 3 * ff), (h, o, w, w, w, w), tokens * ff)[0]


def mlp_back(h, o, by_y, w, ff, extra):
    (tokens, d), heads, n = h.shape, o.shape[0], w.shape[0]
    size = (3 * ff + d) // n + (0 if extra is None else extra.shape[1])
    more = [] if extra is None else [extra]
    return _call(functools.partial(_mlp_back, extra=extra is not None), tokens,
                 [_rows(d), _heads(heads), _rows(d)] + _matrices(w, d, ff) + [_whole(e.shape, 0, 0, 0) for e in more],
                 [_rows(d), _heads(heads), pl.BlockSpec((heads, TOKENS), lambda i: (0, i)), _whole((n, size, d), 0, 0, 0)],
                 [jax.ShapeDtypeStruct((tokens, d), BF16), jax.ShapeDtypeStruct((heads, tokens, HEAD), BF16),
                  jax.ShapeDtypeStruct((heads, tokens), F32), jax.ShapeDtypeStruct((n, size, d), BF16)],
                 [pltpu.VMEM((d, ff), F32)] * 3 + [pltpu.VMEM((heads * HEAD, d), F32)],
                 2 * tokens * d * (3 * d + 8 * ff), (h, o, by_y, w, w, w, w, *more), tokens * ff)


def qkv_back(h, by_q, by_k, by_v, turn, w, number, by_h):
    (tokens, d), heads, n = h.shape, by_q.shape[0], w.shape[0]
    rows = d // n
    last = by_h is None
    specs = [_rows(d)] + [_heads(heads)] * 3 + [_rows(HEAD)] * 2
    args = [h, by_q, by_k, by_v, *turn]
    outs, shapes = [_whole((n, 3 * rows, d), 0, 0, 0)], [jax.ShapeDtypeStruct((n, 3 * rows, d), BF16)]
    if not last:
        specs += [_whole((n, 3 * rows, d), 0, number, 0), _rows(d)]
        args += [w, by_h]
        outs, shapes = [_rows(d)] + outs, [jax.ShapeDtypeStruct((tokens, d), BF16)] + shapes
    got = _call(functools.partial(_qkv_back, last=last), tokens, specs, outs, shapes, [pltpu.VMEM((3, d, heads * HEAD), F32)],
                (6 if last else 12) * tokens * d * d, args)
    return (None, got[0]) if last else got


def _place(n):
    me = lax.axis_index("dp")
    return lax.div(me, CORES), lax.rem(me, CORES), n // CORES


def _greet(others, meanwhile=lambda: None):
    barrier = pltpu.get_barrier_semaphore()
    for other in others:
        pl.semaphore_signal(barrier, inc=1, device_id={"dp": other}, device_id_type=MESH)
    meanwhile()
    pl.semaphore_wait(barrier, len(others))


def _send(src, dst, sems, i, to):
    copy = pltpu.make_async_remote_copy(src_ref=src, dst_ref=dst, send_sem=sems[0].at[i], recv_sem=sems[1].at[i], device_id={"dp": to},
                                        device_id_type=MESH)
    copy.start()
    return copy


def _gather(x_ref, out_ref, right_send, right_recv, left_send, left_recv, pair_send, pair_recv, own_sem):
    n = out_ref.shape[0]
    chip, core, chips = _place(n)
    at = lambda c, k: lax.rem(c + 2 * chips, chips) * CORES + k
    me, partner = at(chip, core), at(chip, 1 - core)
    right, left = at(chip + 1, core), at(chip - 1, core)
    _greet((left, right, partner))
    own = pltpu.make_async_copy(x_ref, out_ref.at[me], own_sem)
    own.start()
    ways = ((right, (right_send, right_recv), chips // 2, -1), (left, (left_send, left_recv), (chips - 1) // 2, 1))
    moving = [[_send(x_ref, out_ref.at[me], sems, 0, to)] for to, sems, _, _ in ways]
    pairs = [_send(x_ref, out_ref.at[me], (pair_send, pair_recv), 0, partner)]
    for step in range(1, chips // 2 + 1):
        for (to, sems, last, sign), copies in zip(ways, moving):
            if step <= last:
                came = out_ref.at[at(chip + sign * step, core)]
                copies[step - 1].wait_recv()
                if step < last:
                    copies.append(_send(came, came, sems, step, to))
                pairs.append(_send(came, came, (pair_send, pair_recv), len(pairs), partner))
    for copy in pairs:
        copy.wait()
    for copies in moving:
        for copy in copies:
            copy.wait_send()
    own.wait()


def gather(x, n):
    chips = n // CORES
    dma = pltpu.SemaphoreType.DMA
    near, far = max((chips - 1) // 2, 1), chips // 2
    vmem = pl.BlockSpec(memory_space=pltpu.VMEM)
    return pl.pallas_call(
        _gather,
        in_specs=[vmem],
        out_specs=vmem,
        out_shape=jax.ShapeDtypeStruct((n, *x.shape), x.dtype),
        scratch_shapes=[dma((far,)), dma((far,)), dma((near,)), dma((near,)), dma((chips,)), dma((chips,)), dma],
        compiler_params=pltpu.CompilerParams(collective_id=1, has_side_effects=True, vmem_limit_bytes=ROOM),
        cost_estimate=pl.CostEstimate(flops=2 * 10**9, transcendentals=0, bytes_accessed=n * x.size * 2),
    )(x)


def _scatter(x_ref, out_ref, pair_s, right_s, left_s, right_in, left_in, pair_send, pair_recv, right_send, right_recv, left_send, left_recv):
    n = x_ref.shape[0]
    chip, core, chips = _place(n)
    at = lambda c, k: lax.rem(c + 2 * chips, chips) * CORES + k
    partner, right, left = at(chip, 1 - core), at(chip + 1, core), at(chip - 1, core)
    far, near = chips // 2, (chips - 1) // 2
    _greet((left, right, partner))
    order = []
    for step in range(far):
        order.append(far - step)
        if step < near:
            order.append(step - near)
    order.append(0)
    pairs = [_send(x_ref.at[at(chip + away, 1 - core)], pair_s.at[i], (pair_send, pair_recv), i, partner) for i, away in enumerate(order)]

    def term(away):
        i = order.index(away)
        pairs[i].wait_recv()
        return x_ref[at(chip + away, core)].astype(F32) + pair_s[i].astype(F32)

    rights, lefts = [], []
    for step in range(far):
        total = term(far - step)
        if step:
            rights[-1].wait_recv()
            total = total + right_in[step - 1].astype(F32)
        right_s[step] = total.astype(BF16)
        rights.append(_send(right_s.at[step], right_in.at[step], (right_send, right_recv), step, right))
        if step < near:
            total = term(step - near)
            if step:
                lefts[-1].wait_recv()
                total = total + left_in[step - 1].astype(F32)
            left_s[step] = total.astype(BF16)
            lefts.append(_send(left_s.at[step], left_in.at[step], (left_send, left_recv), step, left))
    total = term(0)
    if lefts:
        lefts[-1].wait_recv()
        total = total + left_in[near - 1].astype(F32)
    rights[-1].wait_recv()
    total = total + right_in[far - 1].astype(F32)
    out_ref[...] = total.astype(BF16)
    for copy in (*pairs, *rights, *lefts):
        copy.wait_send()


def scatter(x):
    n, *block = x.shape
    chips = n // CORES
    far, near = chips // 2, max((chips - 1) // 2, 1)
    dma = pltpu.SemaphoreType.DMA
    vmem = pl.BlockSpec(memory_space=pltpu.VMEM)
    room = lambda count: pltpu.VMEM((count, *block), BF16)
    return pl.pallas_call(
        _scatter,
        in_specs=[vmem],
        out_specs=vmem,
        out_shape=jax.ShapeDtypeStruct(tuple(block), BF16),
        scratch_shapes=[room(chips), room(far), room(near), room(far), room(near)] + [dma((chips,))] * 2 + [dma((far,))] * 2 + [dma((near,))] * 2,
        compiler_params=pltpu.CompilerParams(collective_id=2, has_side_effects=True, vmem_limit_bytes=ROOM),
        cost_estimate=pl.CostEstimate(flops=10**9, transcendentals=0, bytes_accessed=2 * x.size),
    )(x)


def _squares(*refs, n):
    *block_refs, out_ref, mine, sums, send_sem, recv_sem = refs
    me = lax.axis_index("dp")
    others = [lax.rem(me + i, n) for i in range(1, n)]

    def add():
        total = jnp.zeros((8, 128), F32)
        for ref in block_refs:
            x = ref[...].astype(F32)
            x = jnp.sum((x * x).reshape(-1, 8, x.shape[1]), axis=0)
            for at in range(0, x.shape[1], 128):
                total = total + x[:, at : at + 128]
        mine[...] = total

    _greet(others, add)
    copies = [_send(mine, sums.at[i], (send_sem, recv_sem), i, other) for i, other in enumerate(others)]
    total = mine[...]
    for i, copy in enumerate(copies):
        copy.wait_recv()
        total = total + sums[i]
    for copy in copies:
        copy.wait_send()
    out_ref[...] = total


def squares(blocks, n):
    vmem = pl.BlockSpec(memory_space=pltpu.VMEM)
    dma = pltpu.SemaphoreType.DMA
    return pl.pallas_call(
        functools.partial(_squares, n=n),
        in_specs=[vmem] * len(blocks),
        out_specs=vmem,
        out_shape=jax.ShapeDtypeStruct((8, 128), F32),
        scratch_shapes=[pltpu.VMEM((8, 128), F32), pltpu.VMEM((n - 1, 8, 128), F32), dma((n - 1,)), dma((n - 1,))],
        compiler_params=pltpu.CompilerParams(collective_id=3, has_side_effects=True),
        cost_estimate=pl.CostEstimate(flops=10**8, transcendentals=0, bytes_accessed=2 * sum(b.size for b in blocks)),
    )(*blocks)


def _adamw(total_ref, *refs, count, places):
    kinds, layers = len(places), len(places[0])
    sums, refs = refs[: len(refs) - 6 * kinds], refs[len(refs) - 6 * kinds :]
    total = jnp.sum(jnp.sum(total_ref[...], axis=0, keepdims=True), axis=1, keepdims=True)
    factor = factor_of(total, count)

    def one(layer):
        for i in range(kinds):
            w_ref, m_ref, v_ref, new_w, new_m, new_v = refs[i::kinds]
            which, row = places[i][layer]
            rows, columns = w_ref.shape[1:]
            width = sums[which].shape[1]
            for c in range(columns // width):
                here = slice(c * width, (c + 1) * width)
                g = sums[which][row + c * rows : row + (c + 1) * rows, :].astype(F32) * factor
                w = w_ref[0, :, here].astype(F32)
                m = 0.9 * m_ref[0, :, here] + 0.1 * g
                v = 0.95 * v_ref[0, :, here] + 0.05 * g * g
                new_m[0, :, here] = m
                new_v[0, :, here] = v
                new_w[0, :, here] = (w - 0.02 * (m * lax.rsqrt(v + 1e-8) + 0.1 * w)).astype(BF16)

    for layer in range(layers):
        pl.when(pl.program_id(0) == layer)(functools.partial(one, layer))


def adamw(total, sums, weights, m, v, places, count):
    own = [pl.BlockSpec((1, *w.shape[1:]), lambda i: (i, 0, 0)) for w in weights]
    like = lambda arrays: [jax.ShapeDtypeStruct(a.shape, a.dtype) for a in arrays]
    size = sum(w.size for w in weights)
    return pl.pallas_call(
        functools.partial(_adamw, count=count, places=places),
        grid=(len(places[0]),),
        in_specs=[_whole(a.shape, *([0] * a.ndim)) for a in (total, *sums)] + own * 3,
        out_specs=own * 3,
        out_shape=like(weights) + like(m) + like(v),
        compiler_params=pltpu.CompilerParams(dimension_semantics=("arbitrary",), vmem_limit_bytes=ROOM),
        cost_estimate=pl.CostEstimate(flops=20 * size, transcendentals=size, bytes_accessed=24 * size),
    )(total, *sums, *weights, *m, *v)


def factor_of(sum_of_squares, count):
    return jnp.minimum(1.0, 0.5 * lax.rsqrt(sum_of_squares / count + 1e-30))


def _pack(*refs, layers):
    kinds = len(NAMES)
    weights, outs = refs[:kinds], refs[kinds:]
    rows, d = weights[0].shape[1:]

    def three(out, at, layer):
        for i in range(3):
            out[at + i * rows : at + (i + 1) * rows, :] = weights[i][layer]
        return at + 3 * rows

    three(outs[0], 0, 0)
    for layer, out in enumerate(outs[1:]):
        at = 0
        for ref in weights[4:]:
            for c in range(0, ref.shape[2], d):
                out[at : at + ref.shape[1], :] = ref[layer, :, c : c + d]
                at += ref.shape[1]
        if layer < layers - 1:
            at = three(out, at, layer + 1)
        out[at:, :] = weights[3][layer]


def pack(weights):
    layers, rows, d = weights[0].shape
    size = sum(w.size for w in weights[3:]) // (layers * d)
    shapes = [(3 * rows, d)] + [(size + (3 * rows if i < layers - 1 else 0), d) for i in range(layers)]
    return pl.pallas_call(
        functools.partial(_pack, layers=layers),
        grid=(1,),
        in_specs=[_whole(w.shape, 0, 0, 0) for w in weights],
        out_specs=[_whole(s, 0, 0) for s in shapes],
        out_shape=[jax.ShapeDtypeStruct(s, BF16) for s in shapes],
        compiler_params=pltpu.CompilerParams(dimension_semantics=("arbitrary",)),
        cost_estimate=pl.CostEstimate(flops=10**6, transcendentals=0, bytes_accessed=4 * sum(w.size for w in weights)),
    )(*weights)


def solution(mesh):
    def step(x, dy, *arrays):
        weights, m, v = (arrays[i : i + 7] for i in (0, 7, 14))
        layers, rows, d = weights[0].shape
        deep = weights[6].shape[1]
        n = mesh.shape["dp"]
        ff = deep * n
        wide = ff // d * rows
        turn = tables(x.shape[1], THETA)
        local, *others = pack(weights)
        rest = [lax.all_gather(t, "dp", axis=0, tiled=False) for t in others]
        firsts = [(gather(local, n), 0)] + [(t, (2 * wide + deep) // (3 * rows)) for t in rest]
        h, kept = x[0], []
        for i in range(layers):
            q, k, val = qkv(h, *firsts[i], turn)
            o, lse = attend(q, k, val)
            kept.append((h, q, k, val, o, lse))
            if i < layers - 1:
                h = mlp(h, o, rest[i], ff)
        by_h, extra = dy[0], None
        blocks, sums = {}, []
        for i in reversed(range(layers)):
            h, q, k, val, o, lse = kept[i]
            by_mid, by_o, delta, grads = mlp_back(h, o, by_h, rest[i], ff, extra)
            if sums:
                by_o, sums[-1] = lax.optimization_barrier((by_o, sums[-1]))
            sums.append(lax.psum_scatter(grads, "dp", scatter_dimension=0, tiled=False))
            by_q, by_k, by_v = attend_back(q, k, val, by_o, lse, delta)
            by_h, extra = qkv_back(h, by_q, by_k, by_v, turn, *firsts[i], by_mid if i else None)
        sums.append(scatter(extra))
        row = {"w_gate": 0, "w_up": wide, "w_down": 2 * wide, "wo": 2 * wide + deep}
        places = []
        for name in NAMES:
            if name in row:
                places.append([(layers - 1 - i, row[name]) for i in range(layers)])
            else:
                places.append([(layers - i, sums[layers - i].shape[0] - 3 * rows + NAMES.index(name) * rows) for i in range(layers)])
        return tuple(adamw(squares(sums, n), sums, weights, m, v, places, n * sum(w.size for w in weights)))

    states, cut_ = P(("rep", "dp"), None, None), P(None, "dp", None)
    return jax.shard_map(
        step,
        mesh=mesh,
        in_specs=(states, states) + (cut_,) * 21,
        out_specs=(P("rep", "dp", None),) * 21,
        check_vma=False,
    )
```
